64 devices in a mesh: rep: 8 (over x, y, core), dp: 8 (over z).
Axes of the slice: x: 2, y: 2, z: 8, core: 2. Of those that a mesh axis runs over, the one named last changes fastest.
The devices are a block of a 4x4x8 slice.
Arguments:
- g_w_gate: bfloat16 [64, 2, 512, 3072], P(('rep', 'dp')), parts along dimension 0
- g_w_up: bfloat16 [64, 2, 512, 3072], P(('rep', 'dp')), parts along dimension 0
- g_w_down: bfloat16 [64, 2, 3072, 512], P(('rep', 'dp')), parts along dimension 0
- w_gate: bfloat16 [2, 512, 3072], replicated
- w_up: bfloat16 [2, 512, 3072], replicated
- w_down: bfloat16 [2, 3072, 512], replicated
- m_w_gate: float32 [2, 512, 3072], P(None, 'dp')
- m_w_up: float32 [2, 512, 3072], P(None, 'dp')
- m_w_down: float32 [2, 3072, 512], P(None, 'dp')
- v_w_gate: float32 [2, 512, 3072], P(None, 'dp')
- v_w_up: float32 [2, 512, 3072], P(None, 'dp')
- v_w_down: float32 [2, 3072, 512], P(None, 'dp')
Outputs:
- output 1: bfloat16 [16, 512, 3072], P('rep'), parts along dimension 0
- output 2: bfloat16 [16, 512, 3072], P('rep'), parts along dimension 0
- output 3: bfloat16 [16, 3072, 512], P('rep'), parts along dimension 0
- output 4: float32 [16, 512, 3072], P('rep', 'dp'), parts along dimension 0
- output 5: float32 [16, 512, 3072], P('rep', 'dp'), parts along dimension 0
- output 6: float32 [16, 3072, 512], P('rep', 'dp'), parts along dimension 0
- output 7: float32 [16, 512, 3072], P('rep', 'dp'), parts along dimension 0
- output 8: float32 [16, 512, 3072], P('rep', 'dp'), parts along dimension 0
- output 9: float32 [16, 3072, 512], P('rep', 'dp'), parts along dimension 0
There are 8 independent parts. The reference program is written for one: setup_inputs(seed, part) draws one part's arguments, and reference() takes and returns one part's arrays. A program takes and returns all parts, laid end to end along the dimension named above; an argument that names none is the same for every part.
All inputs are finite; a program needn't handle non-finite values.
Results may differ from the reference program's by a relative error of at most 0.022.
Values are sent between devices in bfloat16 or wider.
A program may use at most 768 MiB of HBM per device.

```python
import jax
import jax.numpy as jnp
from jax import lax

DEVICES = 8
D = 512
FF = 3072
LAYERS = 2
NAMES = ("w_gate", "w_up", "w_down")
SHAPES = {"w_gate": (LAYERS, D, FF), "w_up": (LAYERS, D, FF), "w_down": (LAYERS, FF, D)}


def setup_inputs(seed: int = 0, part: int = 0) -> dict:
    kz, *keys = jax.random.split(jax.random.key(seed), 1 + 5 * len(NAMES))
    loud = 2.0 ** jax.random.uniform(kz, (), jnp.float32, -1.0, 1.0)
    drawn = {}
    for name, key, both in zip(NAMES, keys[:3], keys[3:6], strict=True):
        own = jax.random.normal(jax.random.fold_in(key, part), (DEVICES, *SHAPES[name]), jnp.float32)
        shared = jax.random.normal(jax.random.fold_in(both, part), SHAPES[name], jnp.float32)
        drawn["g_" + name] = (loud * (0.7 * shared / DEVICES + 0.7 * own * DEVICES**-0.5)).astype(jnp.bfloat16)
    for name, key in zip(NAMES, keys[6:9], strict=True):
        drawn[name] = (jax.random.normal(key, SHAPES[name], jnp.float32) * SHAPES[name][1] ** -0.5).astype(jnp.bfloat16)
    for name, key in zip(NAMES, keys[9:12], strict=True):
        drawn["m_" + name] = loud * 0.5 * jax.random.normal(key, SHAPES[name], jnp.float32)
    for name, key in zip(NAMES, keys[12:15], strict=True):
        drawn["v_" + name] = loud * loud * jax.random.uniform(key, SHAPES[name], jnp.float32, 0.5, 1.5)
    return drawn


def adamw(w, m, v, g):
    m = 0.9 * m + 0.1 * g
    v = 0.95 * v + 0.05 * g * g
    step = m * lax.rsqrt(v + 1e-8) + 0.1 * w
    return (w - 0.02 * step).astype(jnp.bfloat16), m, v


def reference(g_w_gate, g_w_up, g_w_down, w_gate, w_up, w_down, m_w_gate, m_w_up, m_w_down, v_w_gate, v_w_up, v_w_down):
    def total(terms):
        return lax.scan(lambda so_far, term: (so_far + term.astype(jnp.float32), None), jnp.zeros(terms.shape[1:], jnp.float32), terms)[0]

    gradients = [total(terms).astype(jnp.bfloat16).astype(jnp.float32) for terms in (g_w_gate, g_w_up, g_w_down)]
    new = [
        adamw(w.astype(jnp.float32), m, v, g)
        for w, m, v, g in zip((w_gate, w_up, w_down), (m_w_gate, m_w_up, m_w_down), (v_w_gate, v_w_up, v_w_down), gradients, strict=True)
    ]
    return tuple(one[which] for which in range(3) for one in new)
```

```python
import functools

import jax
import jax.numpy as jnp
from jax import lax
from jax.experimental import pallas as pl
from jax.experimental.pallas import tpu as pltpu
from jax.sharding import PartitionSpec as P

MESH = pl.DeviceIdType.MESH
F32, BF16 = jnp.float32, jnp.bfloat16
ROWS, COLS = 16, 512
AHEAD = 3
LAG = 16000


def adamw(w, m, v, g):
    m = 0.9 * m + 0.1 * g
    v = 0.95 * v + 0.05 * g * g
    step = m * lax.rsqrt(v + 1e-8) + 0.1 * w
    return (w - 0.02 * step).astype(BF16), m, v


def tiles(shape, body):
    across = shape[1] // COLS

    @pl.loop(0, (shape[0] // ROWS) * across)
    def _(i):
        r = pl.multiple_of((i // across) * ROWS, ROWS)
        c = pl.multiple_of((i % across) * COLS, COLS)
        body(pl.ds(r, ROWS), pl.ds(c, COLS))


class Ring:
    def __init__(self, axis, n):
        self.axis, self.n = axis, n
        self.me = lax.axis_index(axis)
        self.target = (lax.rem(self.me + 1, n), lax.rem(self.me + n - 1, n))

    def greet(self):
        barrier = pltpu.get_barrier_semaphore()
        for neighbour in self.target:
            pl.semaphore_signal(barrier, inc=1, device_id={self.axis: neighbour}, device_id_type=MESH)
        pl.semaphore_wait(barrier, 2)

    def start_of(self, d, hops, rows):
        owner = lax.rem(self.me + (-1, 1)[d] * hops + 2 * self.n, self.n)
        return pl.multiple_of(owner * rows, rows)

    def copy(self, d, src, dst, send, recv):
        return pltpu.make_async_remote_copy(
            src_ref=src, dst_ref=dst, send_sem=send, recv_sem=recv,
            device_id={self.axis: self.target[d]}, device_id_type=MESH,
        )


def first_kernel(n, axis, groups, *refs):
    it = iter(refs)
    take = lambda k: [next(it) for _ in range(k)]
    g_hbm, w_hbm, m_hbm, v_hbm = take(3), take(3), take(3), take(3)
    w_out, m_out, v_out = take(3), take(3), take(3)
    slots, terms, own = take(3), take(3), take(3)
    rs_send, rs_recv, ag_send, ag_recv, term_sem, state_sem = take(6)

    ring = Ring(axis, n)
    rows = [w.shape[1] for w in own]
    pairs = [(q, d) for q in range(3) for d in range(2)]
    last = n - 2

    def block(d, hops, q):
        return pl.ds(ring.start_of(d, hops, rows[q]), rows[q])

    def rs_copy(q, d, s, src):
        return ring.copy(d, src, slots[q].at[d, s], rs_send.at[q, d, s], rs_recv.at[q, d, s])

    def ag_copy(q, d, s):
        ref = w_out[q].at[d, block(d, s, q)]
        return ring.copy(d, ref, ref, ag_send.at[q, d, s], ag_recv.at[q, d, s])

    def term_copy(q, d, s):
        slot = lax.rem(s, AHEAD)
        return pltpu.make_async_copy(g_hbm[q].at[d, block(d, s + 2, q)], terms[q].at[d, slot], term_sem.at[q, d, slot])

    def state_copies(q):
        return (
            pltpu.make_async_copy(w_hbm[q].at[:, block(0, 0, q)], own[q], state_sem.at[q, 0]),
            pltpu.make_async_copy(m_hbm[q], m_out[q], state_sem.at[q, 1]),
            pltpu.make_async_copy(v_hbm[q], v_out[q], state_sem.at[q, 2]),
        )

    ring.greet()
    if LAG:
        @pl.when(lax.rem(lax.axis_index(groups), 2) == 1)
        def _():
            pl.delay(LAG)

    for q, d in pairs:
        rs_copy(q, d, 0, g_hbm[q].at[d, block(d, 1, q)]).start()
    for s in range(AHEAD):
        for q, d in pairs:
            term_copy(q, d, s).start()
    for q in range(3):
        for c in state_copies(q):
            c.start()

    @pl.loop(0, last)
    def _(s):
        for q, d in pairs:
            slot = slots[q].at[d, s]
            term = terms[q].at[d, lax.rem(s, AHEAD)]
            rs_copy(q, d, s, slot).wait_recv()
            term_copy(q, d, s).wait()

            def add(r, c):
                slot[r, c] = (slot[r, c].astype(F32) + term[r, c].astype(F32)).astype(BF16)

            tiles(term.shape, add)
            rs_copy(q, d, s + 1, slot).start()

            @pl.when(s + AHEAD < n - 1)
            def _():
                term_copy(q, d, s + AHEAD).start()

    for q in range(3):
        for c in state_copies(q):
            c.wait()
    for q, d in pairs:
        slot, term = slots[q].at[d, last], terms[q].at[d, last % AHEAD]
        base = ring.start_of(0, 0, rows[q])
        rs_copy(q, d, last, slot).wait_recv()
        term_copy(q, d, last).wait()

        def update(r, c):
            g = (slot[r, c].astype(F32) + term[r, c].astype(F32)).astype(BF16).astype(F32)
            w, m, v = adamw(own[q][d, r, c].astype(F32), m_out[q][d, r, c], v_out[q][d, r, c], g)
            w_out[q][d, pl.ds(pl.multiple_of(base + r.start, ROWS), ROWS), c] = w
            m_out[q][d, r, c] = m
            v_out[q][d, r, c] = v

        tiles(term.shape, update)
        ag_copy(q, d, 0).start()

    @pl.loop(0, last - 1)
    def _(s):
        for q, d in pairs:
            ag_copy(q, d, s).wait_recv()
            ag_copy(q, d, s + 1).start()

    for q, d in pairs:
        ag_copy(q, d, last - 1).wait_recv()

    @pl.loop(0, last)
    def _(s):
        for q, d in pairs:
            rs_copy(q, d, s, slots[q].at[d, s]).wait_send()
            ag_copy(q, d, s).wait_send()

    for q, d in pairs:
        rs_copy(q, d, last, slots[q].at[d, last]).wait_send()


def second_kernel(n, axis, *refs):
    w, out, send, recv = refs[:3], refs[3:6], refs[6], refs[7]
    ring = Ring(axis, n)
    rows = [o.shape[1] for o in out]
    copies = [
        ring.copy(d, w[q].at[d, pl.ds(ring.start_of(d, n - 2, rows[q]), rows[q])], out[q].at[d], send.at[q, d], recv.at[q, d])
        for q in range(3)
        for d in range(2)
    ]
    ring.greet()
    for c in copies:
        c.start()
    for c in copies:
        c.wait()


def out_kernel(*refs):
    k = len(refs) // 2
    copies = [pltpu.make_async_copy(refs[i], refs[k + i], refs[-1].at[i]) for i in range(k)]
    for c in copies:
        c.start()
    for c in copies:
        c.wait()


def written(*arrays):
    return pl.pallas_call(
        out_kernel,
        out_shape=tuple(jax.ShapeDtypeStruct(a.shape, a.dtype) for a in arrays),
        in_specs=[pl.BlockSpec(memory_space=pltpu.VMEM)] * len(arrays),
        out_specs=tuple([pl.BlockSpec(memory_space=pltpu.HBM)] * len(arrays)),
        scratch_shapes=[pltpu.SemaphoreType.DMA((len(arrays),))],
        compiler_params=pltpu.CompilerParams(vmem_limit_bytes=2**20, has_side_effects=True),
    )(*arrays)


def last_kernel(n, axis, *refs):
    blocks, out, sem = refs[:3], refs[6:9], refs[9]
    ring = Ring(axis, n)
    copies = []
    for q in range(3):
        rows = blocks[q].shape[1]
        for d in range(2):
            there = out[q].at[d, pl.ds(ring.start_of(d, n - 1, rows), rows)]
            copies.append(pltpu.make_async_copy(blocks[q].at[d], there, sem.at[q, d]))
    for c in copies:
        c.start()
    for c in copies:
        c.wait()


def solution(mesh):
    groups, axis = "rep", "dp"
    n = mesh.shape[axis]
    dma = pltpu.SemaphoreType.DMA
    vmem, hbm = pl.BlockSpec(memory_space=pltpu.VMEM), pl.BlockSpec(memory_space=pltpu.HBM)

    def step(*arrays):
        terms, weights, m, v = (arrays[i : i + 3] for i in (0, 3, 6, 9))
        terms = [t[0] for t in terms]
        shares = [(one.shape[1], one.shape[2]) for one in m]
        whole = [pltpu.VMEM(w.shape, BF16) for w in weights]
        state = [pltpu.VMEM(one.shape, F32) for one in (*m, *v)]
        results = pl.pallas_call(
            functools.partial(first_kernel, n, axis, groups),
            out_shape=(*whole, *state),
            in_specs=[hbm] * 12,
            out_specs=tuple([vmem] * 9),
            scratch_shapes=[
                *[pltpu.VMEM((2, n - 1, *s), BF16) for s in shares],
                *[pltpu.VMEM((2, AHEAD, *s), BF16) for s in shares],
                *[pltpu.VMEM((2, *s), BF16) for s in shares],
                *[dma((3, 2, n - 1))] * 2,
                *[dma((3, 2, n - 2))] * 2,
                dma((3, 2, AHEAD)),
                dma((3, 3)),
            ],
            compiler_params=pltpu.CompilerParams(
                collective_id=0, has_side_effects=True, vmem_limit_bytes=30 * 2**20
            ),
        )(*terms, *weights, *m, *v)
        first = written(*results)
        gathered, first = lax.optimization_barrier((results[:3], first))
        blocks = pl.pallas_call(
            functools.partial(second_kernel, n, axis),
            out_shape=tuple(pltpu.VMEM((2, *s), BF16) for s in shares),
            in_specs=[vmem] * 3,
            out_specs=tuple([vmem] * 3),
            scratch_shapes=[dma((3, 2))] * 2,
            compiler_params=pltpu.CompilerParams(
                collective_id=1, has_side_effects=True, vmem_limit_bytes=2**20
            ),
        )(*gathered)
        complete = pl.pallas_call(
            functools.partial(last_kernel, n, axis),
            out_shape=tuple(jax.ShapeDtypeStruct(w.shape, BF16) for w in weights),
            in_specs=[vmem] * 3 + [hbm] * 3,
            out_specs=tuple([hbm] * 3),
            scratch_shapes=[dma((3, 2))],
            input_output_aliases={3: 0, 4: 1, 5: 2},
            compiler_params=pltpu.CompilerParams(vmem_limit_bytes=2**20, has_side_effects=True),
        )(*blocks, *first[:3])
        return (*complete, *first[3:])

    all_of, cut = P(None, None, None), P(None, "dp", None)
    return jax.shard_map(
        step,
        mesh=mesh,
        in_specs=(P(("rep", "dp"), None, None, None),) * 3 + (all_of,) * 3 + (cut,) * 6,
        out_specs=(P("rep", None, None),) * 3 + (P("rep", "dp", None),) * 6,
        check_vma=False,
    )
```

```python
import functools

import jax
import jax.numpy as jnp
from jax import lax
from jax.experimental import pallas as pl
from jax.experimental.pallas import tpu as pltpu
from jax.sharding import PartitionSpec as P

MESH = pl.DeviceIdType.MESH
F32, BF16 = jnp.float32, jnp.bfloat16
ROWS, COLS = 16, 512
AHEAD = 3
LATE = (1, 1, 2)
LAG = 18000


def adamw(w, m, v, g):
    m = 0.9 * m + 0.1 * g
    v = 0.95 * v + 0.05 * g * g
    step = m * lax.rsqrt(v + 1e-8) + 0.1 * w
    return (w - 0.02 * step).astype(BF16), m, v


def tiles(shape, body):
    across = shape[1] // COLS

    @pl.loop(0, (shape[0] // ROWS) * across)
    def _(i):
        r = pl.multiple_of((i // across) * ROWS, ROWS)
        c = pl.multiple_of((i % across) * COLS, COLS)
        body(pl.ds(r, ROWS), pl.ds(c, COLS))


class Ring:
    def __init__(self, axis, n):
        self.axis, self.n = axis, n
        self.me = lax.axis_index(axis)
        self.target = (lax.rem(self.me + 1, n), lax.rem(self.me + n - 1, n))

    def greet(self):
        barrier = pltpu.get_barrier_semaphore()
        for neighbour in self.target:
            pl.semaphore_signal(barrier, inc=1, device_id={self.axis: neighbour}, device_id_type=MESH)
        pl.semaphore_wait(barrier, 2)

    def start_of(self, d, hops, rows):
        owner = lax.rem(self.me + (-1, 1)[d] * hops + 2 * self.n, self.n)
        return pl.multiple_of(owner * rows, rows)

    def copy(self, d, src, dst, send, recv):
        return pltpu.make_async_remote_copy(
            src_ref=src, dst_ref=dst, send_sem=send, recv_sem=recv,
            device_id={self.axis: self.target[d]}, device_id_type=MESH,
        )


def first_kernel(n, axis, groups, *refs):
    it = iter(refs)
    take = lambda k: [next(it) for _ in range(k)]
    g_hbm, w_hbm, m_hbm, v_hbm = take(3), take(3), take(3), take(3)
    w_out, m_out, v_out = take(3), take(3), take(3)
    slots, terms, own = take(3), take(3), take(3)
    rs_send, rs_recv, ag_send, ag_recv, term_sem, state_sem = take(6)

    ring = Ring(axis, n)
    rows = [w.shape[1] for w in own]
    pairs = [(q, d) for q in range(3) for d in range(2)]
    last = n - 2

    def block(d, hops, q):
        return pl.ds(ring.start_of(d, hops, rows[q]), rows[q])

    def rs_copy(q, d, s, src):
        return ring.copy(d, src, slots[q].at[d, s], rs_send.at[q, d, s], rs_recv.at[q, d, s])

    def ag_copy(q, d, s):
        ref = w_out[q].at[d, block(d, s, q)]
        return ring.copy(d, ref, ref, ag_send.at[q, d, s], ag_recv.at[q, d, s])

    def term_copy(q, d, s):
        slot = lax.rem(s, AHEAD)
        return pltpu.make_async_copy(g_hbm[q].at[d, block(d, s + 2, q)], terms[q].at[d, slot], term_sem.at[q, d, slot])

    def state_copies(q):
        return (
            pltpu.make_async_copy(w_hbm[q].at[:, block(0, 0, q)], own[q], state_sem.at[q, 0]),
            pltpu.make_async_copy(m_hbm[q], m_out[q], state_sem.at[q, 1]),
            pltpu.make_async_copy(v_hbm[q], v_out[q], state_sem.at[q, 2]),
        )

    ring.greet()
    if LAG:
        @pl.when(lax.rem(lax.axis_index(groups), 2) == 1)
        def _():
            pl.delay(LAG)

    for q, d in pairs:
        rs_copy(q, d, 0, g_hbm[q].at[d, block(d, 1, q)]).start()
    for s in range(AHEAD):
        for q, d in pairs:
            term_copy(q, d, s).start()

    @pl.loop(0, last)
    def _(s):
        @pl.when(s == 1)
        def _():
            for q in range(3):
                for c in state_copies(q):
                    c.start()

        for q, d in pairs:
            slot = slots[q].at[d, s]
            term = terms[q].at[d, lax.rem(s, AHEAD)]
            rs_copy(q, d, s, slot).wait_recv()
            term_copy(q, d, s).wait()

            def add(r, c):
                slot[r, c] = (slot[r, c].astype(F32) + term[r, c].astype(F32)).astype(BF16)

            tiles(term.shape, add)
            rs_copy(q, d, s + 1, slot).start()

            @pl.when(s + AHEAD < n - 1)
            def _():
                term_copy(q, d, s + AHEAD).start()

            @pl.when(s > 0)
            def _():
                rs_copy(q, d, s - 1, slots[q].at[d, s - 1]).wait_send()

    for q in range(3):
        for c in state_copies(q):
            c.wait()
    for q, d in pairs:
        slot, term = slots[q].at[d, last], terms[q].at[d, last % AHEAD]
        base = ring.start_of(0, 0, rows[q])
        rs_copy(q, d, last, slot).wait_recv()
        term_copy(q, d, last).wait()

        def update(r, c):
            g = (slot[r, c].astype(F32) + term[r, c].astype(F32)).astype(BF16).astype(F32)
            w, m, v = adamw(own[q][d, r, c].astype(F32), m_out[q][d, r, c], v_out[q][d, r, c], g)
            w_out[q][d, pl.ds(pl.multiple_of(base + r.start, ROWS), ROWS), c] = w
            m_out[q][d, r, c] = m
            v_out[q][d, r, c] = v

        tiles(term.shape, update)
        ag_copy(q, d, 0).start()

    steps = [n - 1 - k for k in LATE]

    @pl.loop(0, min(steps) - 1)
    def _(s):
        for q, d in pairs:
            ag_copy(q, d, s).wait_recv()
            ag_copy(q, d, s + 1).start()

            @pl.when(s > 0)
            def _():
                ag_copy(q, d, s - 1).wait_send()

            @pl.when(s < 2)
            def _():
                rs_copy(q, d, last - 1 + s, slots[q].at[d, last]).wait_send()

    for s in range(min(steps) - 1, max(steps)):
        for q, d in pairs:
            if s < steps[q]:
                ag_copy(q, d, s).wait_recv()
            if s + 1 < steps[q]:
                ag_copy(q, d, s + 1).start()
    for q, d in pairs:
        for s in range(min(steps) - 2, steps[q]):
            ag_copy(q, d, s).wait_send()


def second_kernel(n, axis, *refs):
    w, out, send, recv = refs[:3], refs[3:6], refs[6], refs[7]
    ring = Ring(axis, n)

    def copy(q, d, j):
        rows = out[q].shape[2]
        src = out[q].at[d, j - 1] if j else w[q].at[d, pl.ds(ring.start_of(d, n - 1 - LATE[q], rows), rows)]
        return ring.copy(d, src, out[q].at[d, j], send.at[q, d, j], recv.at[q, d, j])

    ring.greet()
    for j in range(max(LATE)):
        for q in sorted(range(3), key=lambda q: -LATE[q]):
            for d in range(2):
                if j < LATE[q]:
                    if j:
                        copy(q, d, j - 1).wait_recv()
                    copy(q, d, j).start()
    for q in range(3):
        for d in range(2):
            for j in range(LATE[q]):
                copy(q, d, j).wait_send()
            copy(q, d, LATE[q] - 1).wait_recv()


def out_kernel(*refs):
    k = len(refs) // 2
    copies = [pltpu.make_async_copy(refs[i], refs[k + i], refs[-1].at[i]) for i in range(k)]
    for c in copies:
        c.start()
    for c in copies:
        c.wait()


def written(*arrays):
    return pl.pallas_call(
        out_kernel,
        out_shape=tuple(jax.ShapeDtypeStruct(a.shape, a.dtype) for a in arrays),
        in_specs=[pl.BlockSpec(memory_space=pltpu.VMEM)] * len(arrays),
        out_specs=tuple([pl.BlockSpec(memory_space=pltpu.HBM)] * len(arrays)),
        scratch_shapes=[pltpu.SemaphoreType.DMA((len(arrays),))],
        compiler_params=pltpu.CompilerParams(vmem_limit_bytes=2**20, has_side_effects=True),
    )(*arrays)


def last_kernel(n, axis, *refs):
    blocks, out, sem = refs[:3], refs[6:9], refs[9]
    ring = Ring(axis, n)
    copies = []
    for q in range(3):
        rows = blocks[q].shape[2]
        for d in range(2):
            for j in range(LATE[q]):
                there = out[q].at[d, pl.ds(ring.start_of(d, n - LATE[q] + j, rows), rows)]
                copies.append(pltpu.make_async_copy(blocks[q].at[d, j], there, sem.at[q, d, j]))
    for c in copies:
        c.start()
    for c in copies:
        c.wait()


def solution(mesh):
    groups, axis = "rep", "dp"
    n = mesh.shape[axis]
    dma = pltpu.SemaphoreType.DMA
    vmem, hbm = pl.BlockSpec(memory_space=pltpu.VMEM), pl.BlockSpec(memory_space=pltpu.HBM)

    def step(*arrays):
        terms, weights, m, v = (arrays[i : i + 3] for i in (0, 3, 6, 9))
        terms = [t[0] for t in terms]
        shares = [(one.shape[1], one.shape[2]) for one in m]
        whole = [pltpu.VMEM(w.shape, BF16) for w in weights]
        state = [pltpu.VMEM(one.shape, F32) for one in (*m, *v)]
        results = pl.pallas_call(
            functools.partial(first_kernel, n, axis, groups),
            out_shape=(*whole, *state),
            in_specs=[hbm] * 12,
            out_specs=tuple([vmem] * 9),
            scratch_shapes=[
                *[pltpu.VMEM((2, n - 1, *s), BF16) for s in shares],
                *[pltpu.VMEM((2, AHEAD, *s), BF16) for s in shares],
                *[pltpu.VMEM((2, *s), BF16) for s in shares],
                *[dma((3, 2, n - 1))] * 4,
                dma((3, 2, AHEAD)),
                dma((3, 3)),
            ],
            compiler_params=pltpu.CompilerParams(
                collective_id=0, has_side_effects=True, vmem_limit_bytes=30 * 2**20
            ),
        )(*terms, *weights, *m, *v)
        first = written(*results)
        gathered, first = lax.optimization_barrier((results[:3], first))
        blocks = pl.pallas_call(
            functools.partial(second_kernel, n, axis),
            out_shape=tuple(pltpu.VMEM((2, k, *s), BF16) for k, s in zip(LATE, shares, strict=True)),
            in_specs=[vmem] * 3,
            out_specs=tuple([vmem] * 3),
            scratch_shapes=[dma((3, 2, max(LATE)))] * 2,
            compiler_params=pltpu.CompilerParams(
                collective_id=1, has_side_effects=True, vmem_limit_bytes=2**20
            ),
        )(*gathered)
        complete = pl.pallas_call(
            functools.partial(last_kernel, n, axis),
            out_shape=tuple(jax.ShapeDtypeStruct(w.shape, BF16) for w in weights),
            in_specs=[vmem] * 3 + [hbm] * 3,
            out_specs=tuple([hbm] * 3),
            scratch_shapes=[dma((3, 2, max(LATE)))],
            input_output_aliases={3: 0, 4: 1, 5: 2},
            compiler_params=pltpu.CompilerParams(vmem_limit_bytes=2**20, has_side_effects=True),
        )(*blocks, *first[:3])
        return (*complete, *first[3:])

    all_of, cut = P(None, None, None), P(None, "dp", None)
    return jax.shard_map(
        step,
        mesh=mesh,
        in_specs=(P(("rep", "dp"), None, None, None),) * 3 + (all_of,) * 3 + (cut,) * 6,
        out_specs=(P("rep", None, None),) * 3 + (P("rep", "dp", None),) * 6,
        check_vma=False,
    )
```

```python
import functools

import jax
import jax.numpy as jnp
from jax import lax
from jax.experimental import pallas as pl
from jax.experimental.pallas import tpu as pltpu
from jax.sharding import PartitionSpec as P

MESH = pl.DeviceIdType.MESH
F32, BF16 = jnp.float32, jnp.bfloat16
ROWS, COLS = 16, 512
AHEAD = 3
LATE = (1, 1, 2)
LAG = 5000


def adamw(w, m, v, g):
    m = 0.9 * m + 0.1 * g
    v = 0.95 * v + 0.05 * g * g
    step = m * lax.rsqrt(v + 1e-8) + 0.1 * w
    return (w - 0.02 * step).astype(BF16), m, v


def is_odd(groups):
    return lax.rem(lax.axis_index(groups), 2) == 1


def tiles(shape, body):
    across = shape[1] // COLS

    @pl.loop(0, (shape[0] // ROWS) * across)
    def _(i):
        r = pl.multiple_of((i // across) * ROWS, ROWS)
        c = pl.multiple_of((i % across) * COLS, COLS)
        body(pl.ds(r, ROWS), pl.ds(c, COLS))


class Ring:
    def __init__(self, axis, n):
        self.axis, self.n = axis, n
        self.me = lax.axis_index(axis)
        self.target = (lax.rem(self.me + 1, n), lax.rem(self.me + n - 1, n))

    def greet(self):
        barrier = pltpu.get_barrier_semaphore()
        for neighbour in self.target:
            pl.semaphore_signal(barrier, inc=1, device_id={self.axis: neighbour}, device_id_type=MESH)
        pl.semaphore_wait(barrier, 2)

    def start_of(self, d, hops, rows):
        owner = lax.rem(self.me + (-1, 1)[d] * hops + 2 * self.n, self.n)
        return pl.multiple_of(owner * rows, rows)

    def copy(self, d, src, dst, send, recv):
        return pltpu.make_async_remote_copy(
            src_ref=src, dst_ref=dst, send_sem=send, recv_sem=recv,
            device_id={self.axis: self.target[d]}, device_id_type=MESH,
        )


def first_kernel(n, axis, groups, *refs):
    it = iter(refs)
    take = lambda k: [next(it) for _ in range(k)]
    g_hbm, w_hbm, m_hbm, v_hbm = take(3), take(3), take(3), take(3)
    w_out, m_out, v_out = take(3), take(3), take(3)
    slots, terms, own = take(3), take(3), take(3)
    rs_send, rs_recv, ag_send, ag_recv, term_sem, state_sem = take(6)

    ring = Ring(axis, n)
    rows = [w.shape[1] for w in own]
    pairs = [(q, d) for q in range(3) for d in range(2)]
    last = n - 2
    odd = is_odd(groups)

    def block(d, hops, q):
        return pl.ds(ring.start_of(d, hops, rows[q]), rows[q])

    def rs_copy(q, d, s, src):
        return ring.copy(d, src, slots[q].at[d, s], rs_send.at[q, d, s], rs_recv.at[q, d, s])

    def ag_copy(q, d, s):
        ref = w_out[q].at[d, block(d, s, q)]
        return ring.copy(d, ref, ref, ag_send.at[q, d, s], ag_recv.at[q, d, s])

    def term_copy(q, d, s):
        slot = lax.rem(s, AHEAD)
        return pltpu.make_async_copy(g_hbm[q].at[d, block(d, s + 2, q)], terms[q].at[d, slot], term_sem.at[q, d, slot])

    def state_copies(q):
        return (
            pltpu.make_async_copy(w_hbm[q].at[:, block(0, 0, q)], own[q], state_sem.at[q, 0]),
            pltpu.make_async_copy(m_hbm[q], m_out[q], state_sem.at[q, 1]),
            pltpu.make_async_copy(v_hbm[q], v_out[q], state_sem.at[q, 2]),
        )

    ring.greet()
    if LAG:
        pl.when(odd)(lambda: pl.delay(LAG))

    for q, d in pairs:
        rs_copy(q, d, 0, g_hbm[q].at[d, block(d, 1, q)]).start()
    for s in range(AHEAD):
        for q, d in pairs:
            term_copy(q, d, s).start()

    @pl.loop(0, last)
    def _(s):
        @pl.when(s == 1)
        def _():
            for q in range(3):
                for c in state_copies(q):
                    c.start()

        for q, d in pairs:
            slot = slots[q].at[d, s]
            term = terms[q].at[d, lax.rem(s, AHEAD)]
            rs_copy(q, d, s, slot).wait_recv()
            term_copy(q, d, s).wait()

            def add(r, c):
                slot[r, c] = (slot[r, c].astype(F32) + term[r, c].astype(F32)).astype(BF16)

            tiles(term.shape, add)
            rs_copy(q, d, s + 1, slot).start()

            @pl.when(s + AHEAD < n - 1)
            def _():
                term_copy(q, d, s + AHEAD).start()

            @pl.when(s > 0)
            def _():
                rs_copy(q, d, s - 1, slots[q].at[d, s - 1]).wait_send()

    for q in range(3):
        for c in state_copies(q):
            c.wait()
    for q, d in pairs:
        slot, term = slots[q].at[d, last], terms[q].at[d, last % AHEAD]
        base = ring.start_of(0, 0, rows[q])
        rs_copy(q, d, last, slot).wait_recv()
        term_copy(q, d, last).wait()

        def update(r, c):
            g = (slot[r, c].astype(F32) + term[r, c].astype(F32)).astype(BF16).astype(F32)
            w, m, v = adamw(own[q][d, r, c].astype(F32), m_out[q][d, r, c], v_out[q][d, r, c], g)
            w_out[q][d, pl.ds(pl.multiple_of(base + r.start, ROWS), ROWS), c] = w
            m_out[q][d, r, c] = m
            v_out[q][d, r, c] = v

        tiles(term.shape, update)
        ag_copy(q, d, 0).start()

    steps = [n - 1 - k for k in LATE]

    @pl.loop(0, min(steps) - 1)
    def _(s):
        for q, d in pairs:
            ag_copy(q, d, s).wait_recv()
            ag_copy(q, d, s + 1).start()

            @pl.when(s > 0)
            def _():
                ag_copy(q, d, s - 1).wait_send()

            @pl.when(s < 2)
            def _():
                rs_copy(q, d, last - 1 + s, slots[q].at[d, last]).wait_send()

    for s in range(min(steps) - 1, max(steps)):
        for q, d in pairs:
            if s < steps[q]:
                ag_copy(q, d, s).wait_recv()
            if s + 1 < steps[q]:
                ag_copy(q, d, s + 1).start()
            elif s + 1 == steps[q]:
                pl.when(odd)(lambda: ag_copy(q, d, s + 1).start())
    for q, d in pairs:
        for s in range(min(steps) - 2, steps[q]):
            ag_copy(q, d, s).wait_send()

    @pl.when(odd)
    def _():
        for q, d in pairs:
            ag_copy(q, d, steps[q]).wait()


def second_kernel(n, axis, groups, *refs):
    w, out, send, recv = refs[:3], refs[3:6], refs[6], refs[7]
    ring = Ring(axis, n)
    odd = is_odd(groups)

    def copy(q, d, j, first):
        rows = out[q].shape[2]
        hops = n - 1 - LATE[q] + j
        src = w[q].at[d, pl.ds(ring.start_of(d, hops, rows), rows)] if j == first else out[q].at[d, j - 1]
        return ring.copy(d, src, out[q].at[d, j], send.at[q, d, j], recv.at[q, d, j])

    def gather(first):
        for j in range(first, max(LATE)):
            for q in sorted(range(3), key=lambda q: -LATE[q]):
                for d in range(2):
                    if j < LATE[q]:
                        if j > first:
                            copy(q, d, j - 1, first).wait_recv()
                        copy(q, d, j, first).start()
        for q in range(3):
            for d in range(2):
                for j in range(first, LATE[q]):
                    copy(q, d, j, first).wait_send()
                if LATE[q] > first:
                    copy(q, d, LATE[q] - 1, first).wait_recv()

    ring.greet()
    pl.when(odd)(lambda: gather(1))
    pl.when(jnp.logical_not(odd))(lambda: gather(0))


def out_kernel(*refs):
    k = len(refs) // 2
    copies = [pltpu.make_async_copy(refs[i], refs[k + i], refs[-1].at[i]) for i in range(k)]
    for c in copies:
        c.start()
    for c in copies:
        c.wait()


def written(*arrays):
    return pl.pallas_call(
        out_kernel,
        out_shape=tuple(jax.ShapeDtypeStruct(a.shape, a.dtype) for a in arrays),
        in_specs=[pl.BlockSpec(memory_space=pltpu.VMEM)] * len(arrays),
        out_specs=tuple([pl.BlockSpec(memory_space=pltpu.HBM)] * len(arrays)),
        scratch_shapes=[pltpu.SemaphoreType.DMA((len(arrays),))],
        compiler_params=pltpu.CompilerParams(vmem_limit_bytes=2**20, has_side_effects=True),
    )(*arrays)


def last_kernel(n, axis, groups, *refs):
    blocks, out, sem = refs[:3], refs[6:9], refs[9]
    ring = Ring(axis, n)
    odd = is_odd(groups)

    def write(first):
        copies = []
        for q in range(3):
            rows = blocks[q].shape[2]
            for d in range(2):
                for j in range(first, LATE[q]):
                    there = out[q].at[d, pl.ds(ring.start_of(d, n - LATE[q] + j, rows), rows)]
                    copies.append(pltpu.make_async_copy(blocks[q].at[d, j], there, sem.at[q, d, j]))
        for c in copies:
            c.start()
        for c in copies:
            c.wait()

    pl.when(odd)(lambda: write(1))
    pl.when(jnp.logical_not(odd))(lambda: write(0))


def solution(mesh):
    groups, axis = "rep", "dp"
    n = mesh.shape[axis]
    dma = pltpu.SemaphoreType.DMA
    vmem, hbm = pl.BlockSpec(memory_space=pltpu.VMEM), pl.BlockSpec(memory_space=pltpu.HBM)

    def step(*arrays):
        terms, weights, m, v = (arrays[i : i + 3] for i in (0, 3, 6, 9))
        terms = [t[0] for t in terms]
        shares = [(one.shape[1], one.shape[2]) for one in m]
        whole = [pltpu.VMEM(w.shape, BF16) for w in weights]
        state = [pltpu.VMEM(one.shape, F32) for one in (*m, *v)]
        results = pl.pallas_call(
            functools.partial(first_kernel, n, axis, groups),
            out_shape=(*whole, *state),
            in_specs=[hbm] * 12,
            out_specs=tuple([vmem] * 9),
            scratch_shapes=[
                *[pltpu.VMEM((2, n - 1, *s), BF16) for s in shares],
                *[pltpu.VMEM((2, AHEAD, *s), BF16) for s in shares],
                *[pltpu.VMEM((2, *s), BF16) for s in shares],
                *[dma((3, 2, n - 1))] * 4,
                dma((3, 2, AHEAD)),
                dma((3, 3)),
            ],
            compiler_params=pltpu.CompilerParams(
                collective_id=0, has_side_effects=True, vmem_limit_bytes=30 * 2**20
            ),
        )(*terms, *weights, *m, *v)
        first = written(*results)
        gathered, first = lax.optimization_barrier((results[:3], first))
        blocks = pl.pallas_call(
            functools.partial(second_kernel, n, axis, groups),
            out_shape=tuple(pltpu.VMEM((2, k, *s), BF16) for k, s in zip(LATE, shares, strict=True)),
            in_specs=[vmem] * 3,
            out_specs=tuple([vmem] * 3),
            scratch_shapes=[dma((3, 2, max(LATE)))] * 2,
            compiler_params=pltpu.CompilerParams(
                collective_id=1, has_side_effects=True, vmem_limit_bytes=2**20
            ),
        )(*gathered)
        complete = pl.pallas_call(
            functools.partial(last_kernel, n, axis, groups),
            out_shape=tuple(jax.ShapeDtypeStruct(w.shape, BF16) for w in weights),
            in_specs=[vmem] * 3 + [hbm] * 3,
            out_specs=tuple([hbm] * 3),
            scratch_shapes=[dma((3, 2, max(LATE)))],
            input_output_aliases={3: 0, 4: 1, 5: 2},
            compiler_params=pltpu.CompilerParams(vmem_limit_bytes=2**20, has_side_effects=True),
        )(*blocks, *first[:3])
        return (*complete, *first[3:])

    all_of, cut = P(None, None, None), P(None, "dp", None)
    return jax.shard_map(
        step,
        mesh=mesh,
        in_specs=(P(("rep", "dp"), None, None, None),) * 3 + (all_of,) * 3 + (cut,) * 6,
        out_specs=(P("rep", None, None),) * 3 + (P("rep", "dp", None),) * 6,
        check_vma=False,
    )
```

```python
import functools

import jax
import jax.numpy as jnp
from jax import lax
from jax.experimental import pallas as pl
from jax.experimental.pallas import tpu as pltpu
from jax.sharding import PartitionSpec as P

MESH = pl.DeviceIdType.MESH
F32, BF16 = jnp.float32, jnp.bfloat16
ROWS, COLS = 16, 512
AHEAD = 3
LATE = (1, 1, 2)
SHARE = 4
LAG = 3000


def adamw(w, m, v, g):
    m = 0.9 * m + 0.1 * g
    v = 0.95 * v + 0.05 * g * g
    step = m * lax.rsqrt(v + 1e-8) + 0.1 * w
    return (w - 0.02 * step).astype(BF16), m, v


def is_odd(groups):
    return lax.rem(lax.axis_index(groups), 2) == 1


def tiles(shape, body):
    across = shape[1] // COLS

    @pl.loop(0, (shape[0] // ROWS) * across)
    def _(i):
        r = pl.multiple_of((i // across) * ROWS, ROWS)
        c = pl.multiple_of((i % across) * COLS, COLS)
        body(pl.ds(r, ROWS), pl.ds(c, COLS))


class Ring:
    def __init__(self, axis, n):
        self.axis, self.n = axis, n
        self.me = lax.axis_index(axis)
        self.target = (lax.rem(self.me + 1, n), lax.rem(self.me + n - 1, n))

    def greet(self):
        barrier = pltpu.get_barrier_semaphore()
        for neighbour in self.target:
            pl.semaphore_signal(barrier, inc=1, device_id={self.axis: neighbour}, device_id_type=MESH)
        pl.semaphore_wait(barrier, 2)

    def start_of(self, d, hops, rows):
        owner = lax.rem(self.me + (-1, 1)[d] * hops + 2 * self.n, self.n)
        return pl.multiple_of(owner * rows, rows)

    def copy(self, d, src, dst, send, recv):
        return pltpu.make_async_remote_copy(
            src_ref=src, dst_ref=dst, send_sem=send, recv_sem=recv,
            device_id={self.axis: self.target[d]}, device_id_type=MESH,
        )


def first_kernel(n, axis, groups, *refs):
    it = iter(refs)
    take = lambda k: [next(it) for _ in range(k)]
    g_hbm, w_hbm, m_hbm, v_hbm = take(3), take(3), take(3), take(3)
    w_out, m_out, v_out = take(3), take(3), take(3)
    slots, terms, own = take(3), take(3), take(3)
    rs_send, rs_recv, ag_send, ag_recv, term_sem, state_sem = take(6)

    ring = Ring(axis, n)
    rows = [w.shape[1] for w in own]
    pairs = [(q, d) for q in range(3) for d in range(2)]
    last = n - 2
    odd = is_odd(groups)

    def block(d, hops, q):
        return pl.ds(ring.start_of(d, hops, rows[q]), rows[q])

    def rs_copy(q, d, s, src):
        return ring.copy(d, src, slots[q].at[d, s], rs_send.at[q, d, s], rs_recv.at[q, d, s])

    def ag_copy(q, d, s):
        ref = w_out[q].at[d, block(d, s, q)]
        return ring.copy(d, ref, ref, ag_send.at[q, d, s], ag_recv.at[q, d, s])

    def most_copy(d):
        size = rows[2] - rows[2] // SHARE
        ref = w_out[2].at[d, pl.ds(ring.start_of(d, last, rows[2]), size)]
        return ring.copy(d, ref, ref, ag_send.at[2, d, last], ag_recv.at[2, d, last])

    def term_copy(q, d, s):
        slot = lax.rem(s, AHEAD)
        return pltpu.make_async_copy(g_hbm[q].at[d, block(d, s + 2, q)], terms[q].at[d, slot], term_sem.at[q, d, slot])

    def state_copies(q):
        return (
            pltpu.make_async_copy(w_hbm[q].at[:, block(0, 0, q)], own[q], state_sem.at[q, 0]),
            pltpu.make_async_copy(m_hbm[q], m_out[q], state_sem.at[q, 1]),
            pltpu.make_async_copy(v_hbm[q], v_out[q], state_sem.at[q, 2]),
        )

    ring.greet()
    if LAG:
        pl.when(odd)(lambda: pl.delay(LAG))

    for q, d in pairs:
        rs_copy(q, d, 0, g_hbm[q].at[d, block(d, 1, q)]).start()
    for s in range(AHEAD):
        for q, d in pairs:
            term_copy(q, d, s).start()

    @pl.loop(0, last)
    def _(s):
        @pl.when(s == 1)
        def _():
            for q in range(3):
                for c in state_copies(q):
                    c.start()

        for q, d in pairs:
            slot = slots[q].at[d, s]
            term = terms[q].at[d, lax.rem(s, AHEAD)]
            rs_copy(q, d, s, slot).wait_recv()
            term_copy(q, d, s).wait()

            def add(r, c):
                slot[r, c] = (slot[r, c].astype(F32) + term[r, c].astype(F32)).astype(BF16)

            tiles(term.shape, add)
            rs_copy(q, d, s + 1, slot).start()

            @pl.when(s + AHEAD < n - 1)
            def _():
                term_copy(q, d, s + AHEAD).start()

            @pl.when(s > 0)
            def _():
                rs_copy(q, d, s - 1, slots[q].at[d, s - 1]).wait_send()

    for q in range(3):
        for c in state_copies(q):
            c.wait()
    for q, d in pairs:
        slot, term = slots[q].at[d, last], terms[q].at[d, last % AHEAD]
        base = ring.start_of(0, 0, rows[q])
        rs_copy(q, d, last, slot).wait_recv()
        term_copy(q, d, last).wait()

        def update(r, c):
            g = (slot[r, c].astype(F32) + term[r, c].astype(F32)).astype(BF16).astype(F32)
            w, m, v = adamw(own[q][d, r, c].astype(F32), m_out[q][d, r, c], v_out[q][d, r, c], g)
            w_out[q][d, pl.ds(pl.multiple_of(base + r.start, ROWS), ROWS), c] = w
            m_out[q][d, r, c] = m
            v_out[q][d, r, c] = v

        tiles(term.shape, update)
        ag_copy(q, d, 0).start()

    steps = [n - 1 - k for k in LATE]

    @pl.loop(0, min(steps) - 1)
    def _(s):
        for q, d in pairs:
            ag_copy(q, d, s).wait_recv()
            ag_copy(q, d, s + 1).start()

            @pl.when(s > 0)
            def _():
                ag_copy(q, d, s - 1).wait_send()

            @pl.when(s < 2)
            def _():
                rs_copy(q, d, last - 1 + s, slots[q].at[d, last]).wait_send()

    for s in range(min(steps) - 1, max(steps)):
        for q, d in pairs:
            if s < steps[q]:
                ag_copy(q, d, s).wait_recv()
            if s + 1 < steps[q]:
                ag_copy(q, d, s + 1).start()
            elif s + 1 == steps[q]:
                pl.when(odd)(lambda: ag_copy(q, d, s + 1).start())
    for q, d in pairs:
        for s in range(min(steps) - 2, steps[q]):
            ag_copy(q, d, s).wait_send()

    @pl.when(odd)
    def _():
        for d in range(2):
            ag_copy(2, d, steps[2]).wait_recv()
            most_copy(d).start()
        for q, d in pairs:
            if q < 2:
                ag_copy(q, d, steps[q]).wait_recv()
            ag_copy(q, d, steps[q]).wait_send()
        for d in range(2):
            most_copy(d).wait()


def second_kernel(n, axis, groups, *refs):
    w, out, send, recv = refs[:3], refs[3:6], refs[6], refs[7]
    ring = Ring(axis, n)
    odd = is_odd(groups)

    def copy(q, d, j, first):
        rows = out[q].shape[2]
        hops = n - 1 - LATE[q] + j
        part = rows // SHARE if first else rows
        here = pl.ds(rows - part, part)
        there = pl.ds(pl.multiple_of(ring.start_of(d, hops, rows) + rows - part, ROWS), part)
        src = w[q].at[d, there] if j == first else out[q].at[d, j - 1]
        return ring.copy(d, src, out[q].at[d, j, here], send.at[q, d, j], recv.at[q, d, j])

    def gather(first):
        for j in range(first, max(LATE)):
            for q in sorted(range(3), key=lambda q: -LATE[q]):
                for d in range(2):
                    if j < LATE[q]:
                        if j > first:
                            copy(q, d, j - 1, first).wait_recv()
                        copy(q, d, j, first).start()
        for q in range(3):
            for d in range(2):
                for j in range(first, LATE[q]):
                    copy(q, d, j, first).wait_send()
                if LATE[q] > first:
                    copy(q, d, LATE[q] - 1, first).wait_recv()

    ring.greet()
    pl.when(odd)(lambda: gather(1))
    pl.when(jnp.logical_not(odd))(lambda: gather(0))


def out_kernel(*refs):
    k = len(refs) // 2
    copies = [pltpu.make_async_copy(refs[i], refs[k + i], refs[-1].at[i]) for i in range(k)]
    for c in copies:
        c.start()
    for c in copies:
        c.wait()


def written(*arrays):
    return pl.pallas_call(
        out_kernel,
        out_shape=tuple(jax.ShapeDtypeStruct(a.shape, a.dtype) for a in arrays),
        in_specs=[pl.BlockSpec(memory_space=pltpu.VMEM)] * len(arrays),
        out_specs=tuple([pl.BlockSpec(memory_space=pltpu.HBM)] * len(arrays)),
        scratch_shapes=[pltpu.SemaphoreType.DMA((len(arrays),))],
        compiler_params=pltpu.CompilerParams(vmem_limit_bytes=2**20, has_side_effects=True),
    )(*arrays)


def last_kernel(n, axis, groups, *refs):
    blocks, out, sem = refs[:3], refs[6:9], refs[9]
    ring = Ring(axis, n)
    odd = is_odd(groups)

    def write(first):
        copies = []
        for q in range(3):
            rows = blocks[q].shape[2]
            for d in range(2):
                for j in range(first, LATE[q]):
                    part = rows // SHARE if first else rows
                    base = ring.start_of(d, n - LATE[q] + j, rows) + rows - part
                    there = out[q].at[d, pl.ds(pl.multiple_of(base, ROWS), part)]
                    copies.append(pltpu.make_async_copy(blocks[q].at[d, j, pl.ds(rows - part, part)], there, sem.at[q, d, j]))
        for c in copies:
            c.start()
        for c in copies:
            c.wait()

    pl.when(odd)(lambda: write(1))
    pl.when(jnp.logical_not(odd))(lambda: write(0))


def solution(mesh):
    groups, axis = "rep", "dp"
    n = mesh.shape[axis]
    dma = pltpu.SemaphoreType.DMA
    vmem, hbm = pl.BlockSpec(memory_space=pltpu.VMEM), pl.BlockSpec(memory_space=pltpu.HBM)

    def step(*arrays):
        terms, weights, m, v = (arrays[i : i + 3] for i in (0, 3, 6, 9))
        terms = [t[0] for t in terms]
        shares = [(one.shape[1], one.shape[2]) for one in m]
        whole = [pltpu.VMEM(w.shape, BF16) for w in weights]
        state = [pltpu.VMEM(one.shape, F32) for one in (*m, *v)]
        results = pl.pallas_call(
            functools.partial(first_kernel, n, axis, groups),
            out_shape=(*whole, *state),
            in_specs=[hbm] * 12,
            out_specs=tuple([vmem] * 9),
            scratch_shapes=[
                *[pltpu.VMEM((2, n - 1, *s), BF16) for s in shares],
                *[pltpu.VMEM((2, AHEAD, *s), BF16) for s in shares],
                *[pltpu.VMEM((2, *s), BF16) for s in shares],
                *[dma((3, 2, n - 1))] * 4,
                dma((3, 2, AHEAD)),
                dma((3, 3)),
            ],
            compiler_params=pltpu.CompilerParams(
                collective_id=0, has_side_effects=True, vmem_limit_bytes=30 * 2**20
            ),
        )(*terms, *weights, *m, *v)
        first = written(*results)
        gathered, first = lax.optimization_barrier((results[:3], first))
        blocks = pl.pallas_call(
            functools.partial(second_kernel, n, axis, groups),
            out_shape=tuple(pltpu.VMEM((2, k, *s), BF16) for k, s in zip(LATE, shares, strict=True)),
            in_specs=[vmem] * 3,
            out_specs=tuple([vmem] * 3),
            scratch_shapes=[dma((3, 2, max(LATE)))] * 2,
            compiler_params=pltpu.CompilerParams(
                collective_id=1, has_side_effects=True, vmem_limit_bytes=2**20
            ),
        )(*gathered)
        complete = pl.pallas_call(
            functools.partial(last_kernel, n, axis, groups),
            out_shape=tuple(jax.ShapeDtypeStruct(w.shape, BF16) for w in weights),
            in_specs=[vmem] * 3 + [hbm] * 3,
            out_specs=tuple([hbm] * 3),
            scratch_shapes=[dma((3, 2, max(LATE)))],
            input_output_aliases={3: 0, 4: 1, 5: 2},
            compiler_params=pltpu.CompilerParams(vmem_limit_bytes=2**20, has_side_effects=True),
        )(*blocks, *first[:3])
        return (*complete, *first[3:])

    all_of, cut = P(None, None, None), P(None, "dp", None)
    return jax.shard_map(
        step,
        mesh=mesh,
        in_specs=(P(("rep", "dp"), None, None, None),) * 3 + (all_of,) * 3 + (cut,) * 6,
        out_specs=(P("rep", None, None),) * 3 + (P("rep", "dp", None),) * 6,
        check_vma=False,
    )
```

```python
import functools

import jax
import jax.numpy as jnp
from jax import lax
from jax.experimental import pallas as pl
from jax.experimental.pallas import tpu as pltpu
from jax.sharding import PartitionSpec as P

MESH = pl.DeviceIdType.MESH
F32, BF16 = jnp.float32, jnp.bfloat16
ROWS, COLS = 16, 512
AHEAD = 3
LATE = (1, 1, 2)
SHARE = 24
LAG = 2400


def adamw(w, m, v, g):
    m = 0.9 * m + 0.1 * g
    v = 0.95 * v + 0.05 * g * g
    step = m * lax.rsqrt(v + 1e-8) + 0.1 * w
    return (w - 0.02 * step).astype(BF16), m, v


def is_odd(groups):
    return lax.rem(lax.axis_index(groups), 2) == 1


def tiles(shape, body):
    across = shape[1] // COLS

    @pl.loop(0, (shape[0] // ROWS) * across)
    def _(i):
        r = pl.multiple_of((i // across) * ROWS, ROWS)
        c = pl.multiple_of((i % across) * COLS, COLS)
        body(pl.ds(r, ROWS), pl.ds(c, COLS))


class Ring:
    def __init__(self, axis, n):
        self.axis, self.n = axis, n
        self.me = lax.axis_index(axis)
        self.target = (lax.rem(self.me + 1, n), lax.rem(self.me + n - 1, n))

    def greet(self):
        barrier = pltpu.get_barrier_semaphore()
        for neighbour in self.target:
            pl.semaphore_signal(barrier, inc=1, device_id={self.axis: neighbour}, device_id_type=MESH)
        pl.semaphore_wait(barrier, 2)

    def start_of(self, d, hops, rows):
        owner = lax.rem(self.me + (-1, 1)[d] * hops + 2 * self.n, self.n)
        return pl.multiple_of(owner * rows, rows)

    def copy(self, d, src, dst, send, recv):
        return pltpu.make_async_remote_copy(
            src_ref=src, dst_ref=dst, send_sem=send, recv_sem=recv,
            device_id={self.axis: self.target[d]}, device_id_type=MESH,
        )


def first_kernel(n, axis, groups, *refs):
    it = iter(refs)
    take = lambda k: [next(it) for _ in range(k)]
    g_hbm, w_hbm, m_hbm, v_hbm = take(3), take(3), take(3), take(3)
    w_out, m_out, v_out = take(3), take(3), take(3)
    slots, terms, own = take(3), take(3), take(3)
    rs_send, rs_recv, ag_send, ag_recv, term_sem, state_sem = take(6)

    ring = Ring(axis, n)
    rows = [w.shape[1] for w in own]
    pairs = [(q, d) for q in range(3) for d in range(2)]
    last = n - 2
    odd = is_odd(groups)

    def block(d, hops, q):
        return pl.ds(ring.start_of(d, hops, rows[q]), rows[q])

    def rs_copy(q, d, s, src):
        return ring.copy(d, src, slots[q].at[d, s], rs_send.at[q, d, s], rs_recv.at[q, d, s])

    def ag_copy(q, d, s):
        ref = w_out[q].at[d, block(d, s, q)]
        return ring.copy(d, ref, ref, ag_send.at[q, d, s], ag_recv.at[q, d, s])

    def most_copy(d):
        size = rows[2] - rows[2] // SHARE
        ref = w_out[2].at[d, pl.ds(ring.start_of(d, last, rows[2]), size)]
        return ring.copy(d, ref, ref, ag_send.at[2, d, last], ag_recv.at[2, d, last])

    def term_copy(q, d, s):
        slot = lax.rem(s, AHEAD)
        return pltpu.make_async_copy(g_hbm[q].at[d, block(d, s + 2, q)], terms[q].at[d, slot], term_sem.at[q, d, slot])

    def state_copies(q):
        return (
            pltpu.make_async_copy(w_hbm[q].at[:, block(0, 0, q)], own[q], state_sem.at[q, 0]),
            pltpu.make_async_copy(m_hbm[q], m_out[q], state_sem.at[q, 1]),
            pltpu.make_async_copy(v_hbm[q], v_out[q], state_sem.at[q, 2]),
        )

    ring.greet()
    if LAG:
        pl.when(odd)(lambda: pl.delay(LAG))

    for q, d in pairs:
        rs_copy(q, d, 0, g_hbm[q].at[d, block(d, 1, q)]).start()
    for s in range(AHEAD):
        for q, d in pairs:
            term_copy(q, d, s).start()

    @pl.loop(0, last)
    def _(s):
        @pl.when(s == 1)
        def _():
            for q in range(3):
                for c in state_copies(q):
                    c.start()

        for q, d in pairs:
            slot = slots[q].at[d, s]
            term = terms[q].at[d, lax.rem(s, AHEAD)]
            rs_copy(q, d, s, slot).wait_recv()
            term_copy(q, d, s).wait()

            def add(r, c):
                slot[r, c] = (slot[r, c].astype(F32) + term[r, c].astype(F32)).astype(BF16)

            tiles(term.shape, add)
            rs_copy(q, d, s + 1, slot).start()

            @pl.when(s + AHEAD < n - 1)
            def _():
                term_copy(q, d, s + AHEAD).start()

            @pl.when(s > 0)
            def _():
                rs_copy(q, d, s - 1, slots[q].at[d, s - 1]).wait_send()

    for q in range(3):
        for c in state_copies(q):
            c.wait()
    for q, d in pairs:
        slot, term = slots[q].at[d, last], terms[q].at[d, last % AHEAD]
        base = ring.start_of(0, 0, rows[q])
        rs_copy(q, d, last, slot).wait_recv()
        term_copy(q, d, last).wait()

        def update(r, c):
            g = (slot[r, c].astype(F32) + term[r, c].astype(F32)).astype(BF16).astype(F32)
            w, m, v = adamw(own[q][d, r, c].astype(F32), m_out[q][d, r, c], v_out[q][d, r, c], g)
            w_out[q][d, pl.ds(pl.multiple_of(base + r.start, ROWS), ROWS), c] = w
            m_out[q][d, r, c] = m
            v_out[q][d, r, c] = v

        tiles(term.shape, update)
        ag_copy(q, d, 0).start()

    steps = [n - 1 - k for k in LATE]

    @pl.loop(0, min(steps) - 1)
    def _(s):
        for q, d in pairs:
            ag_copy(q, d, s).wait_recv()
            ag_copy(q, d, s + 1).start()

            @pl.when(s > 0)
            def _():
                ag_copy(q, d, s - 1).wait_send()

            @pl.when(s < 2)
            def _():
                rs_copy(q, d, last - 1 + s, slots[q].at[d, last]).wait_send()

    for s in range(min(steps) - 1, max(steps)):
        for q, d in pairs:
            if s < steps[q]:
                ag_copy(q, d, s).wait_recv()
            if s + 1 < steps[q]:
                ag_copy(q, d, s + 1).start()
            elif s + 1 == steps[q]:
                pl.when(odd)(lambda: ag_copy(q, d, s + 1).start())
    for q, d in pairs:
        for s in range(min(steps) - 2, steps[q]):
            ag_copy(q, d, s).wait_send()

    @pl.when(odd)
    def _():
        for d in range(2):
            ag_copy(2, d, steps[2]).wait_recv()
            most_copy(d).start()
        for q, d in pairs:
            if q < 2:
                ag_copy(q, d, steps[q]).wait_recv()
            ag_copy(q, d, steps[q]).wait_send()
        for d in range(2):
            most_copy(d).wait()


def second_kernel(n, axis, groups, *refs):
    w, out, send, recv = refs[:3], refs[3:6], refs[6], refs[7]
    ring = Ring(axis, n)
    odd = is_odd(groups)

    def copy(q, d, j, first):
        rows = out[q].shape[2]
        hops = n - 1 - LATE[q] + j
        part = rows // SHARE if first else rows
        here = pl.ds(rows - part, part)
        there = pl.ds(pl.multiple_of(ring.start_of(d, hops, rows) + rows - part, ROWS), part)
        src = w[q].at[d, there] if j == first else out[q].at[d, j - 1]
        return ring.copy(d, src, out[q].at[d, j, here], send.at[q, d, j], recv.at[q, d, j])

    def gather(first):
        for j in range(first, max(LATE)):
            for q in sorted(range(3), key=lambda q: -LATE[q]):
                for d in range(2):
                    if j < LATE[q]:
                        if j > first:
                            copy(q, d, j - 1, first).wait_recv()
                        copy(q, d, j, first).start()
        for q in range(3):
            for d in range(2):
                for j in range(first, LATE[q]):
                    copy(q, d, j, first).wait_send()
                if LATE[q] > first:
                    copy(q, d, LATE[q] - 1, first).wait_recv()

    ring.greet()
    pl.when(odd)(lambda: gather(1))
    pl.when(jnp.logical_not(odd))(lambda: gather(0))


def out_kernel(*refs):
    k = len(refs) // 2
    copies = [pltpu.make_async_copy(refs[i], refs[k + i], refs[-1].at[i]) for i in range(k)]
    for c in copies:
        c.start()
    for c in copies:
        c.wait()


def written(*arrays):
    return pl.pallas_call(
        out_kernel,
        out_shape=tuple(jax.ShapeDtypeStruct(a.shape, a.dtype) for a in arrays),
        in_specs=[pl.BlockSpec(memory_space=pltpu.VMEM)] * len(arrays),
        out_specs=tuple([pl.BlockSpec(memory_space=pltpu.HBM)] * len(arrays)),
        scratch_shapes=[pltpu.SemaphoreType.DMA((len(arrays),))],
        compiler_params=pltpu.CompilerParams(vmem_limit_bytes=2**20, has_side_effects=True),
    )(*arrays)


def last_kernel(n, axis, groups, *refs):
    blocks, out, sem = refs[:3], refs[6:9], refs[9]
    ring = Ring(axis, n)
    odd = is_odd(groups)

    def write(first):
        copies = []
        for q in range(3):
            rows = blocks[q].shape[2]
            for d in range(2):
                for j in range(first, LATE[q]):
                    part = rows // SHARE if first else rows
                    base = ring.start_of(d, n - LATE[q] + j, rows) + rows - part
                    there = out[q].at[d, pl.ds(pl.multiple_of(base, ROWS), part)]
                    copies.append(pltpu.make_async_copy(blocks[q].at[d, j, pl.ds(rows - part, part)], there, sem.at[q, d, j]))
        for c in copies:
            c.start()
        for c in copies:
            c.wait()

    pl.when(odd)(lambda: write(1))
    pl.when(jnp.logical_not(odd))(lambda: write(0))


def solution(mesh):
    groups, axis = "rep", "dp"
    n = mesh.shape[axis]
    dma = pltpu.SemaphoreType.DMA
    vmem, hbm = pl.BlockSpec(memory_space=pltpu.VMEM), pl.BlockSpec(memory_space=pltpu.HBM)

    def step(*arrays):
        terms, weights, m, v = (arrays[i : i + 3] for i in (0, 3, 6, 9))
        terms = [t[0] for t in terms]
        shares = [(one.shape[1], one.shape[2]) for one in m]
        whole = [pltpu.VMEM(w.shape, BF16) for w in weights]
        state = [pltpu.VMEM(one.shape, F32) for one in (*m, *v)]
        results = pl.pallas_call(
            functools.partial(first_kernel, n, axis, groups),
            out_shape=(*whole, *state),
            in_specs=[hbm] * 12,
            out_specs=tuple([vmem] * 9),
            scratch_shapes=[
                *[pltpu.VMEM((2, n - 1, *s), BF16) for s in shares],
                *[pltpu.VMEM((2, AHEAD, *s), BF16) for s in shares],
                *[pltpu.VMEM((2, *s), BF16) for s in shares],
                *[dma((3, 2, n - 1))] * 4,
                dma((3, 2, AHEAD)),
                dma((3, 3)),
            ],
            compiler_params=pltpu.CompilerParams(
                collective_id=0, has_side_effects=True, vmem_limit_bytes=30 * 2**20
            ),
        )(*terms, *weights, *m, *v)
        first = written(*results)
        gathered, first = lax.optimization_barrier((results[:3], first))
        blocks = pl.pallas_call(
            functools.partial(second_kernel, n, axis, groups),
            out_shape=tuple(pltpu.VMEM((2, k, *s), BF16) for k, s in zip(LATE, shares, strict=True)),
            in_specs=[vmem] * 3,
            out_specs=tuple([vmem] * 3),
            scratch_shapes=[dma((3, 2, max(LATE)))] * 2,
            compiler_params=pltpu.CompilerParams(
                collective_id=1, has_side_effects=True, vmem_limit_bytes=2**20
            ),
        )(*gathered)
        complete = pl.pallas_call(
            functools.partial(last_kernel, n, axis, groups),
            out_shape=tuple(jax.ShapeDtypeStruct(w.shape, BF16) for w in weights),
            in_specs=[vmem] * 3 + [hbm] * 3,
            out_specs=tuple([hbm] * 3),
            scratch_shapes=[dma((3, 2, max(LATE)))],
            input_output_aliases={3: 0, 4: 1, 5: 2},
            compiler_params=pltpu.CompilerParams(vmem_limit_bytes=2**20, has_side_effects=True),
        )(*blocks, *first[:3])
        return (*complete, *first[3:])

    all_of, cut = P(None, None, None), P(None, "dp", None)
    return jax.shard_map(
        step,
        mesh=mesh,
        in_specs=(P(("rep", "dp"), None, None, None),) * 3 + (all_of,) * 3 + (cut,) * 6,
        out_specs=(P("rep", None, None),) * 3 + (P("rep", "dp", None),) * 6,
        check_vma=False,
    )
```
